32 devices in a mesh: pair: 4 (over x, core), ep: 8 (over z, y).
Axes of the slice: x: 2, y: 2, z: 4, core: 2. Of those that a mesh axis runs over, the one named last changes fastest.
Arguments:
- tokens: bfloat16 [8192, 4096], P(('pair', 'ep')), may hold values from -6 to 6
- expert_of: int32 [8192, 1], P(('pair', 'ep')), may hold values from 0 to 31, as said below
- w_gate: bfloat16 [32, 4096, 768], P(('pair', 'ep')), may hold values from -0.09375 to 0.09375
- w_up: bfloat16 [32, 4096, 768], P(('pair', 'ep')), may hold values from -0.09375 to 0.09375
- w_down: bfloat16 [32, 768, 4096], P(('pair', 'ep')), may hold values from -0.21875 to 0.21875
Outputs:
- mixed: bfloat16 [8192, 4096], P(('pair', 'ep'))
The draws below stay inside these ranges and needn't reach their ends.
Inputs may be any that keep to these rules, and one draw needn't show every extreme that they name: `expert_of`: the rows of one device (aligned blocks of 256 tokens) name no expert more than 12 times; in every draw one expert, drawn from the seed, is named exactly 12 times in every device's rows.
All inputs are finite; a program needn't handle non-finite values.
Results may differ from the reference program's by a relative error of at most 0.005.
Values may be sent and summed in bfloat16 or wider, within the bound.
A program may use at most 128 MiB of HBM per device.

```python
import jax
import jax.numpy as jnp
from jax import lax

D = 4096
FF = 768
TOK_DEV = 256
EXPERTS = 32
CAP = 12
TOKENS = 8192


def draw_expert_of(key, part):
    blocks = TOKENS // TOK_DEV
    hottest = jax.random.randint(jax.random.fold_in(key, 7), (), 0, EXPERTS).astype(jnp.int32)
    block_keys = jax.random.split(jax.random.fold_in(key, 11), blocks)

    def one_block(block_key):
        first_key, second_key = jax.random.split(block_key)
        others = jnp.repeat(jnp.arange(EXPERTS - 1, dtype=jnp.int32), CAP)
        others = jax.random.permutation(first_key, others)[:TOK_DEV - CAP]
        others = others + (others >= hottest).astype(jnp.int32)
        block_rows = jnp.concatenate([jnp.full((CAP,), hottest, jnp.int32), others])
        return jax.random.permutation(second_key, block_rows)
    return jax.vmap(one_block)(block_keys).reshape(TOKENS, 1).astype(jnp.int32)


def steps_of(stream_key, dims, shards, least, high):
    def one(dim, blocks):
        steps = jax.random.uniform(jax.random.fold_in(jax.random.fold_in(stream_key, 6), dim), (blocks,), jnp.float32, least / len(shards), high / len(shards))
        return jnp.repeat(jnp.exp(steps), dims[dim] // blocks).reshape((-1,) + (1,) * (len(dims) - dim - 1))

    level = one(*shards[0])
    for cut in shards[1:]:
        level = level * one(*cut)
    return level


def normal_values(stream_key, extent, scale, bound, cuts=(), kind=jnp.bfloat16):
    values = scale * jax.random.normal(stream_key, extent, jnp.float32)
    if cuts:
        values = values * steps_of(stream_key, extent, cuts, -0.22, 0.18)
    return jnp.clip(values, -bound, bound).astype(kind)


def setup_inputs(seed: int = 0) -> dict:
    keys = jax.random.split(jax.random.key(seed), 6)
    return {
        "tokens": normal_values(keys[0], (TOKENS, D), 1.0, 6.0, ((0, 32),)),
        "expert_of": draw_expert_of(jax.random.fold_in(keys[5], 71), 0),
        "w_gate": normal_values(keys[2], (EXPERTS, D, FF), D ** -0.5, 0.09375, ((0, 32),)),
        "w_up": normal_values(keys[3], (EXPERTS, D, FF), D ** -0.5, 0.09375, ((0, 32),)),
        "w_down": normal_values(keys[4], (EXPERTS, FF, D), FF ** -0.5, 0.21875, ((0, 32),)),
    }


def reference(tokens, expert_of, w_gate, w_up, w_down):
    routed = expert_of[:, 0].astype(jnp.int32)
    row_limit = EXPERTS * CAP
    sorted_rows = jnp.argsort(routed, stable=True).astype(jnp.int32)
    expert_load = jnp.sum((routed[:, None] == jnp.arange(EXPERTS, dtype=jnp.int32)[None, :]).astype(jnp.int32), axis=0).astype(jnp.int32)
    offsets = (jnp.cumsum(expert_load) - expert_load).astype(jnp.int32)
    padded_order = jnp.concatenate([sorted_rows, jnp.full((row_limit,), TOKENS, jnp.int32)])

    def per_expert(mixed_sofar, expert):
        picked = lax.dynamic_slice(padded_order, (offsets[expert].astype(jnp.int32),), (row_limit,))
        is_live = jnp.arange(row_limit, dtype=jnp.int32) < expert_load[expert]
        picked = jnp.where(is_live, picked, TOKENS).astype(jnp.int32)
        gathered = jnp.take(tokens, jnp.minimum(picked, TOKENS - 1), axis=0)
        gate_proj = jnp.dot(gathered, w_gate[expert], preferred_element_type=jnp.float32)
        up_proj = jnp.dot(gathered, w_up[expert], preferred_element_type=jnp.float32)
        hidden = (jax.nn.silu(gate_proj) * up_proj).astype(jnp.bfloat16)
        result = jnp.dot(hidden, w_down[expert], preferred_element_type=jnp.float32).astype(jnp.bfloat16)
        return mixed_sofar.at[picked].set(result, mode="drop"), None

    start = jnp.zeros((TOKENS, D), jnp.bfloat16)
    mixed, _ = lax.scan(per_expert, start, jnp.arange(EXPERTS, dtype=jnp.int32))
    return mixed
```

```python
import functools

import jax
import jax.numpy as jnp
from jax import lax
from jax.experimental import pallas as pl
from jax.experimental.pallas import tpu as pltpu
from jax.sharding import PartitionSpec as P

MESH = pl.DeviceIdType.MESH
TILE = 16
GROUP = 8


def dot(a, b):
    return jnp.dot(a, b, preferred_element_type=jnp.float32)


def exchange_ffn(
    pairs, eps, cap, out_ref, gate_hbm, up_hbm, down_hbm, ret_ref,
    recv, result, gate, up, down, hidden, rest,
    w_sem, local_sem, send1, recv1, send2, recv2,
):
    n = pairs * eps
    pair, ep = lax.axis_index("pair"), lax.axis_index("ep")
    me = pair * eps + ep
    width = recv.shape[2]
    tail = rest.shape[1]
    parts = cap // (TILE - cap)
    spare = TILE - cap

    def shift(k):
        i = k // pairs
        de = (eps // 2 + ((i + 1) // 2) * (2 * ((i + 1) % 2) - 1) + eps) % eps
        return (k + 1) % pairs, de

    def target(k):
        dp, de = shift(k)
        return lax.rem(pair + dp, pairs), lax.rem(ep + de, eps)

    def origin(k):
        dp, de = shift(k)
        return lax.rem(pair + pairs - dp, pairs), lax.rem(ep + eps - de, eps)

    loads = [
        pltpu.make_async_copy(src.at[0], dst, w_sem.at[i])
        for i, (src, dst) in enumerate(((gate_hbm, gate), (up_hbm, up), (down_hbm, down)))
    ]
    for load in loads:
        load.start()
    own = pltpu.make_async_copy(out_ref.at[me], recv.at[n - 1], local_sem.at[0])
    own.start()

    barrier = pltpu.get_barrier_semaphore()

    @pl.loop(0, n - 1)
    def _(k):
        p, e = target(k)
        pl.semaphore_signal(barrier, inc=1, device_id=(p, e), device_id_type=MESH)

    pl.semaphore_wait(barrier, n - 1)

    def outbound(k):
        p, e = target(k)
        return pltpu.make_async_remote_copy(
            src_ref=out_ref.at[p * eps + e],
            dst_ref=recv.at[k],
            send_sem=send1.at[k],
            recv_sem=recv1.at[k],
            device_id=(p, e),
            device_id_type=MESH,
        )

    def inbound(k):
        p, e = origin(k)
        return pltpu.make_async_remote_copy(
            src_ref=result.at[k],
            dst_ref=ret_ref.at[me],
            send_sem=send2.at[k],
            recv_sem=recv2.at[me],
            device_id=(p, e),
            device_id_type=MESH,
        )

    @pl.loop(0, n - 1)
    def _(k):
        outbound(k).start()

    for load in loads:
        load.wait()
    own.wait()

    rows = GROUP * TILE
    r = lax.broadcasted_iota(jnp.int32, (rows, rows), 0)
    c = lax.broadcasted_iota(jnp.int32, (rows, rows), 1)
    same = (r // TILE) == (c // TILE)
    r, c = r % TILE, c % TILE

    def unpacker(j):
        pick = same & (r // spare == j) & (c == cap + r % spare)
        return pick.astype(jnp.float32).astype(jnp.bfloat16)

    def packer(j):
        pick = same & (r >= cap) & (c == spare * j + r - cap)
        return pick.astype(jnp.float32).astype(jnp.bfloat16)

    body_row = (lax.broadcasted_iota(jnp.int32, (rows, 1), 0) % TILE) < cap
    step = 256

    @pl.loop(0, n // GROUP)
    def _(g):
        first = g * GROUP

        @pl.loop(0, GROUP)
        def _(i):
            @pl.when(first + i < n - 1)
            def _():
                outbound(first + i).wait_recv()

        block = recv.at[pl.ds(first, GROUP)]
        total = jnp.zeros((rows, tail), jnp.float32)
        for j in range(parts):
            piece = block[:, :, j * tail:(j + 1) * tail].reshape(rows, tail)
            total = total + dot(unpacker(j), piece)
        rest[...] = total.astype(jnp.bfloat16)

        @pl.loop(0, hidden.shape[1] // step)
        def _(f):
            cols = pl.ds(pl.multiple_of(f * step, step), step)
            main = block[...].reshape(rows, width)
            g_out = dot(main, gate[:width, cols]) + dot(rest[...], gate[width:, cols])
            u_out = dot(main, up[:width, cols]) + dot(rest[...], up[width:, cols])
            hidden[:, cols] = (jax.nn.silu(g_out) * u_out).astype(jnp.bfloat16)

        rest[...] = dot(hidden[...], down[:, width:]).astype(jnp.bfloat16)
        for j in range(parts):
            cols = pl.ds(j * tail, tail)
            body = dot(hidden[...], down[:, cols])
            extra = dot(packer(j), rest[...])
            packed = jnp.where(body_row, body, extra).astype(jnp.bfloat16)
            result[pl.ds(first, GROUP), :, cols] = packed.reshape(GROUP, TILE, tail)

        @pl.loop(0, GROUP)
        def _(i):
            @pl.when(first + i < n - 1)
            def _():
                inbound(first + i).start()

    mine = pltpu.make_async_copy(result.at[n - 1], ret_ref.at[me], local_sem.at[1])
    mine.start()
    mine.wait()

    @pl.loop(0, n - 1)
    def _(k):
        outbound(k).wait_send()
        inbound(k).wait_send()
        p, e = target(k)
        peer = p * eps + e
        pltpu.make_async_remote_copy(
            src_ref=result.at[k],
            dst_ref=ret_ref.at[peer],
            send_sem=send2.at[k],
            recv_sem=recv2.at[peer],
            device_id=(p, e),
            device_id_type=MESH,
        ).wait_recv()


def fused(tokens, routed, slot, w_gate, w_up, w_down, pairs, eps, cap):
    n = pairs * eps
    tok_rows, depth = tokens.shape
    ff = w_gate.shape[2]
    spare = TILE - cap
    parts = cap // spare
    tail = depth * spare // TILE
    width = depth - tail

    row = jnp.arange(n * TILE, dtype=jnp.int32)
    key = routed * TILE + slot
    main_sel = key[:, None] == row[None, :]
    rest_key = jnp.where(
        slot[:, None] // spare == jnp.arange(parts)[None, :],
        (routed * TILE + cap + slot % spare)[:, None],
        -1,
    )
    rest_sel = [rest_key[:, j][:, None] == row[None, :] for j in range(parts)]
    main_f = main_sel.astype(jnp.bfloat16)
    rest_f = [s.astype(jnp.bfloat16) for s in rest_sel]
    last = tokens[:, width:]
    pieces = []
    for j in range(parts):
        both = jnp.concatenate([main_f, rest_f[j]], axis=0)
        rows = jnp.concatenate([tokens[:, j * tail:(j + 1) * tail], last], axis=0)
        pieces.append(
            lax.dot_general(
                both, rows, (((0,), (0,)), ((), ())), preferred_element_type=jnp.float32
            ).astype(jnp.bfloat16)
        )
    outgoing = jnp.concatenate(pieces, axis=1).reshape(n, TILE, width)

    vmem = pl.BlockSpec(memory_space=pltpu.VMEM)
    hbm = pl.BlockSpec(memory_space=pl.ANY)
    bf16 = jnp.bfloat16
    returned = pl.pallas_call(
        functools.partial(exchange_ffn, pairs, eps, cap),
        out_shape=jax.ShapeDtypeStruct((n, TILE, width), bf16),
        in_specs=[vmem, hbm, hbm, hbm],
        out_specs=vmem,
        scratch_shapes=[
            pltpu.VMEM((n, TILE, width), bf16),
            pltpu.VMEM((n, TILE, width), bf16),
            pltpu.VMEM((depth, ff), bf16),
            pltpu.VMEM((depth, ff), bf16),
            pltpu.VMEM((ff, depth), bf16),
            pltpu.VMEM((GROUP * TILE, ff), bf16),
            pltpu.VMEM((GROUP * TILE, tail), bf16),
            pltpu.SemaphoreType.DMA((3,)),
            pltpu.SemaphoreType.DMA((2,)),
            pltpu.SemaphoreType.DMA((n,)),
            pltpu.SemaphoreType.DMA((n,)),
            pltpu.SemaphoreType.DMA((n,)),
            pltpu.SemaphoreType.DMA((n,)),
        ],
        compiler_params=pltpu.CompilerParams(
            collective_id=0, has_side_effects=True, vmem_limit_bytes=56 * 1024 * 1024
        ),
        name="exchange_ffn",
    )(outgoing, w_gate, w_up, w_down)
    back = returned.reshape(n * TILE, width)
    head = dot(main_f, back).astype(bf16)
    ends = sum(dot(rest_f[j], back[:, j * tail:(j + 1) * tail]) for j in range(parts))
    return jnp.concatenate([head, ends.astype(bf16)], axis=1)


def plain(tokens, routed, slot, w_gate, w_up, w_down, experts, capacity):
    position = routed * capacity + slot
    outgoing = (
        jnp.zeros((experts * capacity, tokens.shape[1]), jnp.bfloat16).at[position].set(tokens)
    )
    parcel = lax.all_to_all(
        outgoing.reshape(experts, capacity, outgoing.shape[1]),
        ("pair", "ep"), split_axis=0, concat_axis=0, tiled=True,
    )
    flat_rows = parcel.reshape(experts * capacity, parcel.shape[2])
    gate_proj = dot(flat_rows, w_gate[0])
    up_proj = dot(flat_rows, w_up[0])
    hidden = (jax.nn.silu(gate_proj) * up_proj).astype(jnp.bfloat16)
    result = dot(hidden, w_down[0]).astype(jnp.bfloat16)
    returned = lax.all_to_all(
        result.reshape(experts, capacity, result.shape[1]),
        ("pair", "ep"), split_axis=0, concat_axis=0, tiled=True,
    )
    return jnp.take(returned.reshape(experts * capacity, -1), position, axis=0)


def shards(tokens, expert_of, w_gate, w_up, w_down):
    pairs = lax.axis_size("pair")
    eps = lax.axis_size("ep")
    experts = pairs * eps
    tok_rows, depth = tokens.shape
    cap = tok_rows // experts + tok_rows // (2 * experts)
    routed = expert_of[:, 0]
    onehot = (routed[:, None] == jnp.arange(experts, dtype=jnp.int32)[None, :]).astype(jnp.float32)
    order = jnp.arange(tok_rows)
    earlier = (order[:, None] > order[None, :]).astype(jnp.bfloat16)
    before = dot(earlier, onehot.astype(jnp.bfloat16))
    slot = jnp.sum(before * onehot, axis=1).astype(jnp.int32)
    spare = TILE - cap
    packs = 0 < spare <= cap and cap % spare == 0 and (depth * spare) % (TILE * 256) == 0
    if packs and experts % GROUP == 0 and w_gate.shape[2] % 256 == 0:
        return fused(tokens, routed, slot, w_gate, w_up, w_down, pairs, eps, cap)
    return plain(tokens, routed, slot, w_gate, w_up, w_down, experts, cap)


def solution(mesh):
    spec2 = P(("pair", "ep"), None)
    spec3 = P(("pair", "ep"), None, None)
    return jax.shard_map(
        shards,
        mesh=mesh,
        in_specs=(spec2, spec2, spec3, spec3, spec3),
        out_specs=spec2,
        check_vma=False,
    )
```

```python
import functools

import jax
import jax.numpy as jnp
from jax import lax
from jax.experimental import pallas as pl
from jax.experimental.pallas import tpu as pltpu
from jax.sharding import PartitionSpec as P

MESH = pl.DeviceIdType.MESH
TILE = 16
GROUP = 8


def dot(a, b):
    return jnp.dot(a, b, preferred_element_type=jnp.float32)


def exchange_ffn(
    pairs, eps, cap, row_keys, col_keys, tok_hbm, gate_hbm, up_hbm, down_hbm, mixed_ref,
    tok, outgoing, recv, result, returned, gate, up, down, hidden, rest,
    tok_sem, w_sem, local_sem, send1, recv1, send2, recv2,
):
    n = pairs * eps
    pair, ep = lax.axis_index("pair"), lax.axis_index("ep")
    tok_rows = tok.shape[0]
    width = recv.shape[2]
    tail = rest.shape[1]
    parts = cap // (TILE - cap)
    spare = TILE - cap
    rows = GROUP * TILE
    bf16 = jnp.bfloat16

    def shift(k):
        i = k // pairs
        de = (eps // 2 + ((i + 1) // 2) * (2 * ((i + 1) % 2) - 1) + eps) % eps
        return (k + 1) % pairs, de

    def target(k):
        dp, de = shift(k)
        return lax.rem(pair + dp, pairs), lax.rem(ep + de, eps)

    def origin(k):
        dp, de = shift(k)
        return lax.rem(pair + pairs - dp, pairs), lax.rem(ep + eps - de, eps)

    tok_load = pltpu.make_async_copy(tok_hbm, tok, tok_sem.at[0])
    tok_load.start()

    barrier = pltpu.get_barrier_semaphore()

    @pl.loop(0, n - 1)
    def _(k):
        p, e = target(k)
        pl.semaphore_signal(barrier, inc=1, device_id=(p, e), device_id_type=MESH)

    loads = [
        pltpu.make_async_copy(src.at[0], dst, w_sem.at[i])
        for i, (src, dst) in enumerate(((gate_hbm, gate), (up_hbm, up), (down_hbm, down)))
    ]
    for load in loads:
        load.start()

    def outbound(k):
        p, e = target(k)
        return pltpu.make_async_remote_copy(
            src_ref=outgoing.at[k],
            dst_ref=recv.at[k],
            send_sem=send1.at[k],
            recv_sem=recv1.at[k],
            device_id=(p, e),
            device_id_type=MESH,
        )

    def inbound(k):
        p, e = origin(k)
        return pltpu.make_async_remote_copy(
            src_ref=result.at[k],
            dst_ref=returned.at[k],
            send_sem=send2.at[k],
            recv_sem=recv2.at[k],
            device_id=(p, e),
            device_id_type=MESH,
        )

    def row_ids(first, shape, axis):
        at = lax.broadcasted_iota(jnp.int32, shape, axis)
        base = jnp.zeros(shape, jnp.int32)
        for i in range(GROUP):
            p, e = target(first + i)
            base = jnp.where(at // TILE == i, (p * eps + e) * TILE, base)
        return base + at % TILE

    def one_hot(mask):
        return mask.astype(jnp.float32).astype(bf16)

    def pack(first):
        ids = row_ids(first, (rows, tok_rows), 0)
        main = one_hot(row_keys[0:1, :] == ids)
        for j in range(parts):
            cols = pl.ds(j * tail, tail)
            ends = one_hot(row_keys[j + 1:j + 2, :] == ids)
            piece = dot(main, tok[:, cols]) + dot(ends, tok[:, width:])
            outgoing[pl.ds(first, GROUP), :, cols] = piece.astype(bf16).reshape(GROUP, TILE, tail)

    def unpack(first, start):
        ids = row_ids(first, (tok_rows, rows), 1)
        main = one_hot(col_keys[:, 0:1] == ids)
        ends = jnp.zeros((tok_rows, tail), jnp.float32)
        for j in range(parts):
            cols = pl.ds(j * tail, tail)
            piece = returned[pl.ds(first, GROUP), :, cols].reshape(rows, tail)
            head = dot(main, piece).astype(bf16)
            mixed_ref[:, cols] = head if start else mixed_ref[:, cols] + head
            ends = ends + dot(one_hot(col_keys[:, j + 1:j + 2] == ids), piece)
        ends = ends.astype(bf16)
        mixed_ref[:, width:] = ends if start else mixed_ref[:, width:] + ends

    def send(first):
        @pl.loop(0, GROUP)
        def _(i):
            @pl.when(first + i < n - 1)
            def _():
                outbound(first + i).start()

    tok_load.wait()
    pack(0)
    pl.semaphore_wait(barrier, n - 1)
    send(0)

    @pl.loop(1, n // GROUP)
    def _(g):
        pack(g * GROUP)
        send(g * GROUP)

    own = pltpu.make_async_copy(outgoing.at[n - 1], recv.at[n - 1], local_sem.at[0])
    own.start()
    for load in loads:
        load.wait()
    own.wait()

    r = lax.broadcasted_iota(jnp.int32, (rows, rows), 0)
    c = lax.broadcasted_iota(jnp.int32, (rows, rows), 1)
    same = (r // TILE) == (c // TILE)
    r, c = r % TILE, c % TILE

    def spreader(j):
        return one_hot(same & (r // spare == j) & (c == cap + r % spare))

    def folder(j):
        return one_hot(same & (r >= cap) & (c == spare * j + r - cap))

    body_row = (lax.broadcasted_iota(jnp.int32, (rows, 1), 0) % TILE) < cap
    step = 256

    @pl.loop(0, n // GROUP)
    def _(g):
        first = g * GROUP

        @pl.loop(0, GROUP)
        def _(i):
            @pl.when(first + i < n - 1)
            def _():
                outbound(first + i).wait_recv()

        block = recv.at[pl.ds(first, GROUP)]
        total = jnp.zeros((rows, tail), jnp.float32)
        for j in range(parts):
            piece = block[:, :, j * tail:(j + 1) * tail].reshape(rows, tail)
            total = total + dot(spreader(j), piece)
        rest[...] = total.astype(bf16)

        @pl.loop(0, hidden.shape[1] // step)
        def _(f):
            cols = pl.ds(pl.multiple_of(f * step, step), step)
            main = block[...].reshape(rows, width)
            g_out = dot(main, gate[:width, cols]) + dot(rest[...], gate[width:, cols])
            u_out = dot(main, up[:width, cols]) + dot(rest[...], up[width:, cols])
            hidden[:, cols] = (jax.nn.silu(g_out) * u_out).astype(bf16)

        rest[...] = dot(hidden[...], down[:, width:]).astype(bf16)
        for j in range(parts):
            cols = pl.ds(j * tail, tail)
            body = dot(hidden[...], down[:, cols])
            extra = dot(folder(j), rest[...])
            packed = jnp.where(body_row, body, extra).astype(bf16)
            result[pl.ds(first, GROUP), :, cols] = packed.reshape(GROUP, TILE, tail)

        @pl.loop(0, GROUP)
        def _(i):
            @pl.when(first + i < n - 1)
            def _():
                inbound(first + i).start()

    mine = pltpu.make_async_copy(result.at[n - 1], returned.at[n - 1], local_sem.at[1])
    mine.start()
    mine.wait()

    def collect(first):
        @pl.loop(0, GROUP)
        def _(i):
            @pl.when(first + i < n - 1)
            def _():
                inbound(first + i).wait_recv()

    collect(0)
    unpack(0, True)

    @pl.loop(1, n // GROUP)
    def _(g):
        collect(g * GROUP)
        unpack(g * GROUP, False)

    @pl.loop(0, n - 1)
    def _(k):
        outbound(k).wait_send()
        inbound(k).wait_send()


def fused(tokens, routed, slot, w_gate, w_up, w_down, pairs, eps, cap):
    n = pairs * eps
    tok_rows, depth = tokens.shape
    ff = w_gate.shape[2]
    spare = TILE - cap
    parts = cap // spare
    tail = depth * spare // TILE
    width = depth - tail

    rest_key = jnp.where(
        slot[None, :] // spare == jnp.arange(parts)[:, None],
        (routed * TILE + cap + slot % spare)[None, :],
        -1,
    )
    keys = jnp.concatenate([(routed * TILE + slot)[None, :], rest_key], axis=0)

    vmem = pl.BlockSpec(memory_space=pltpu.VMEM)
    hbm = pl.BlockSpec(memory_space=pl.ANY)
    bf16 = jnp.bfloat16
    parcels = pltpu.VMEM((n, TILE, width), bf16)
    return pl.pallas_call(
        functools.partial(exchange_ffn, pairs, eps, cap),
        out_shape=jax.ShapeDtypeStruct((tok_rows, depth), bf16),
        in_specs=[vmem, vmem, hbm, hbm, hbm, hbm],
        out_specs=vmem,
        scratch_shapes=[
            pltpu.VMEM((tok_rows, depth), bf16),
            parcels,
            parcels,
            parcels,
            parcels,
            pltpu.VMEM((depth, ff), bf16),
            pltpu.VMEM((depth, ff), bf16),
            pltpu.VMEM((ff, depth), bf16),
            pltpu.VMEM((GROUP * TILE, ff), bf16),
            pltpu.VMEM((GROUP * TILE, tail), bf16),
            pltpu.SemaphoreType.DMA((1,)),
            pltpu.SemaphoreType.DMA((3,)),
            pltpu.SemaphoreType.DMA((2,)),
            pltpu.SemaphoreType.DMA((n,)),
            pltpu.SemaphoreType.DMA((n,)),
            pltpu.SemaphoreType.DMA((n,)),
            pltpu.SemaphoreType.DMA((n,)),
        ],
        compiler_params=pltpu.CompilerParams(
            collective_id=0, has_side_effects=True, vmem_limit_bytes=56 * 1024 * 1024
        ),
        name="exchange_ffn",
    )(keys, keys.T, tokens, w_gate, w_up, w_down)


def plain(tokens, routed, slot, w_gate, w_up, w_down, experts, capacity):
    position = routed * capacity + slot
    outgoing = (
        jnp.zeros((experts * capacity, tokens.shape[1]), jnp.bfloat16).at[position].set(tokens)
    )
    parcel = lax.all_to_all(
        outgoing.reshape(experts, capacity, outgoing.shape[1]),
        ("pair", "ep"), split_axis=0, concat_axis=0, tiled=True,
    )
    flat_rows = parcel.reshape(experts * capacity, parcel.shape[2])
    gate_proj = dot(flat_rows, w_gate[0])
    up_proj = dot(flat_rows, w_up[0])
    hidden = (jax.nn.silu(gate_proj) * up_proj).astype(jnp.bfloat16)
    result = dot(hidden, w_down[0]).astype(jnp.bfloat16)
    returned = lax.all_to_all(
        result.reshape(experts, capacity, result.shape[1]),
        ("pair", "ep"), split_axis=0, concat_axis=0, tiled=True,
    )
    return jnp.take(returned.reshape(experts * capacity, -1), position, axis=0)


def shards(tokens, expert_of, w_gate, w_up, w_down):
    pairs = lax.axis_size("pair")
    eps = lax.axis_size("ep")
    experts = pairs * eps
    tok_rows, depth = tokens.shape
    cap = tok_rows // experts + tok_rows // (2 * experts)
    routed = expert_of[:, 0]
    onehot = (routed[:, None] == jnp.arange(experts, dtype=jnp.int32)[None, :]).astype(jnp.float32)
    order = jnp.arange(tok_rows)
    earlier = (order[:, None] > order[None, :]).astype(jnp.bfloat16)
    before = dot(earlier, onehot.astype(jnp.bfloat16))
    slot = jnp.sum(before * onehot, axis=1).astype(jnp.int32)
    spare = TILE - cap
    packs = 0 < spare <= cap and cap % spare == 0 and (depth * spare) % (TILE * 256) == 0
    if packs and experts % GROUP == 0 and w_gate.shape[2] % 256 == 0:
        return fused(tokens, routed, slot, w_gate, w_up, w_down, pairs, eps, cap)
    return plain(tokens, routed, slot, w_gate, w_up, w_down, experts, cap)


def solution(mesh):
    spec2 = P(("pair", "ep"), None)
    spec3 = P(("pair", "ep"), None, None)
    return jax.shard_map(
        shards,
        mesh=mesh,
        in_specs=(spec2, spec2, spec3, spec3, spec3),
        out_specs=spec2,
        check_vma=False,
    )
```

```python
import functools

import jax
import jax.numpy as jnp
from jax import lax
from jax.experimental import pallas as pl
from jax.experimental.pallas import tpu as pltpu
from jax.sharding import PartitionSpec as P

MESH = pl.DeviceIdType.MESH
TILE = 16
GROUP = 8


def dot(a, b):
    return jnp.dot(a, b, preferred_element_type=jnp.float32)


def exchange_ffn(
    pairs, eps, cap, row_keys, col_keys, tok_hbm, gate_hbm, up_hbm, down_hbm, head_ref, ends_ref,
    tok, outgoing, recv, result, returned, gate, up, down, hidden, rest,
    tok_sem, w_sem, local_sem, send1, recv1, send2, recv2,
):
    n = pairs * eps
    pair, ep = lax.axis_index("pair"), lax.axis_index("ep")
    tok_rows = tok.shape[0]
    width = recv.shape[2]
    tail = rest.shape[1]
    parts = cap // (TILE - cap)
    spare = TILE - cap
    rows = GROUP * TILE
    bf16 = jnp.bfloat16

    def shift(k):
        i = k // pairs
        de = (eps // 2 + ((i + 1) // 2) * (2 * ((i + 1) % 2) - 1) + eps) % eps
        return (k + 1) % pairs, de

    def target(k):
        dp, de = shift(k)
        return lax.rem(pair + dp, pairs), lax.rem(ep + de, eps)

    def origin(k):
        dp, de = shift(k)
        return lax.rem(pair + pairs - dp, pairs), lax.rem(ep + eps - de, eps)

    tok_load = pltpu.make_async_copy(tok_hbm, tok, tok_sem.at[0])
    tok_load.start()

    barrier = pltpu.get_barrier_semaphore()

    @pl.loop(0, n - 1)
    def _(k):
        p, e = target(k)
        pl.semaphore_signal(barrier, inc=1, device_id=(p, e), device_id_type=MESH)

    loads = [
        pltpu.make_async_copy(src.at[0], dst, w_sem.at[i])
        for i, (src, dst) in enumerate(((gate_hbm, gate), (up_hbm, up), (down_hbm, down)))
    ]
    for load in loads:
        load.start()

    def outbound(k):
        p, e = target(k)
        return pltpu.make_async_remote_copy(
            src_ref=outgoing.at[k],
            dst_ref=recv.at[k],
            send_sem=send1.at[k],
            recv_sem=recv1.at[k],
            device_id=(p, e),
            device_id_type=MESH,
        )

    def inbound(k):
        p, e = origin(k)
        return pltpu.make_async_remote_copy(
            src_ref=result.at[k],
            dst_ref=returned.at[k],
            send_sem=send2.at[k],
            recv_sem=recv2.at[k],
            device_id=(p, e),
            device_id_type=MESH,
        )

    def row_ids(first, shape, axis):
        at = lax.broadcasted_iota(jnp.int32, shape, axis)
        base = jnp.zeros(shape, jnp.int32)
        for i in range(GROUP):
            p, e = target(first + i)
            base = jnp.where(at // TILE == i, (p * eps + e) * TILE, base)
        return base + at % TILE

    def one_hot(mask):
        return mask.astype(jnp.float32).astype(bf16)

    def pack(first):
        ids = row_ids(first, (rows, tok_rows), 0)
        main = one_hot(row_keys[0:1, :] == ids)
        for j in range(parts):
            cols = pl.ds(j * tail, tail)
            ends = one_hot(row_keys[j + 1:j + 2, :] == ids)
            piece = dot(main, tok[:, cols]) + dot(ends, tok[:, width:])
            outgoing[pl.ds(first, GROUP), :, cols] = piece.astype(bf16).reshape(GROUP, TILE, tail)

    def unpack(first, start):
        ids = row_ids(first, (tok_rows, rows), 1)
        main = one_hot(col_keys[:, 0:1] == ids)
        ends = jnp.zeros((tok_rows, tail), jnp.float32)
        for j in range(parts):
            cols = pl.ds(j * tail, tail)
            piece = returned[pl.ds(first, GROUP), :, cols].reshape(rows, tail)
            head = dot(main, piece).astype(bf16)
            head_ref[:, cols] = head if start else head_ref[:, cols] + head
            ends = ends + dot(one_hot(col_keys[:, j + 1:j + 2] == ids), piece)
        ends = ends.astype(bf16)
        ends_ref[...] = ends if start else ends_ref[...] + ends

    def send(first):
        @pl.loop(0, GROUP)
        def _(i):
            @pl.when(first + i < n - 1)
            def _():
                outbound(first + i).start()

    tok_load.wait()
    pack(0)
    pl.semaphore_wait(barrier, n - 1)
    send(0)

    @pl.loop(1, n // GROUP)
    def _(g):
        pack(g * GROUP)
        send(g * GROUP)

    own = pltpu.make_async_copy(outgoing.at[n - 1], recv.at[n - 1], local_sem.at[0])
    own.start()
    for load in loads:
        load.wait()
    own.wait()

    r = lax.broadcasted_iota(jnp.int32, (rows, rows), 0)
    c = lax.broadcasted_iota(jnp.int32, (rows, rows), 1)
    same = (r // TILE) == (c // TILE)
    r, c = r % TILE, c % TILE

    def spreader(j):
        return one_hot(same & (r // spare == j) & (c == cap + r % spare))

    def folder(j):
        return one_hot(same & (r >= cap) & (c == spare * j + r - cap))

    body_row = (lax.broadcasted_iota(jnp.int32, (rows, 1), 0) % TILE) < cap
    step = 256

    @pl.loop(0, n // GROUP)
    def _(g):
        first = g * GROUP

        @pl.loop(0, GROUP)
        def _(i):
            @pl.when(first + i < n - 1)
            def _():
                outbound(first + i).wait_recv()

        block = recv.at[pl.ds(first, GROUP)]
        total = jnp.zeros((rows, tail), jnp.float32)
        for j in range(parts):
            piece = block[:, :, j * tail:(j + 1) * tail].reshape(rows, tail)
            total = total + dot(spreader(j), piece)
        rest[...] = total.astype(bf16)

        @pl.loop(0, hidden.shape[1] // step)
        def _(f):
            cols = pl.ds(pl.multiple_of(f * step, step), step)
            main = block[...].reshape(rows, width)
            g_out = dot(main, gate[:width, cols]) + dot(rest[...], gate[width:, cols])
            u_out = dot(main, up[:width, cols]) + dot(rest[...], up[width:, cols])
            hidden[:, cols] = (jax.nn.silu(g_out) * u_out).astype(bf16)

        rest[...] = dot(hidden[...], down[:, width:]).astype(bf16)
        for j in range(parts):
            cols = pl.ds(j * tail, tail)
            body = dot(hidden[...], down[:, cols])
            extra = dot(folder(j), rest[...])
            packed = jnp.where(body_row, body, extra).astype(bf16)
            result[pl.ds(first, GROUP), :, cols] = packed.reshape(GROUP, TILE, tail)

        @pl.loop(0, GROUP)
        def _(i):
            @pl.when(first + i < n - 1)
            def _():
                inbound(first + i).start()

    mine = pltpu.make_async_copy(result.at[n - 1], returned.at[n - 1], local_sem.at[1])
    mine.start()
    mine.wait()

    def collect(first):
        @pl.loop(0, GROUP)
        def _(i):
            @pl.when(first + i < n - 1)
            def _():
                inbound(first + i).wait_recv()

    collect(0)
    unpack(0, True)

    @pl.loop(1, n // GROUP)
    def _(g):
        collect(g * GROUP)
        unpack(g * GROUP, False)

    @pl.loop(0, n - 1)
    def _(k):
        outbound(k).wait_send()
        inbound(k).wait_send()


def fused(tokens, routed, slot, w_gate, w_up, w_down, pairs, eps, cap):
    n = pairs * eps
    tok_rows, depth = tokens.shape
    ff = w_gate.shape[2]
    spare = TILE - cap
    parts = cap // spare
    tail = depth * spare // TILE
    width = depth - tail

    rest_key = jnp.where(
        slot[None, :] // spare == jnp.arange(parts)[:, None],
        (routed * TILE + cap + slot % spare)[None, :],
        -1,
    )
    keys = jnp.concatenate([(routed * TILE + slot)[None, :], rest_key], axis=0)

    vmem = pl.BlockSpec(memory_space=pltpu.VMEM)
    hbm = pl.BlockSpec(memory_space=pl.ANY)
    bf16 = jnp.bfloat16
    parcels = pltpu.VMEM((n, TILE, width), bf16)
    head, ends = pl.pallas_call(
        functools.partial(exchange_ffn, pairs, eps, cap),
        out_shape=[
            jax.ShapeDtypeStruct((tok_rows, width), bf16),
            jax.ShapeDtypeStruct((tok_rows, tail), bf16),
        ],
        in_specs=[vmem, vmem, hbm, hbm, hbm, hbm],
        out_specs=[vmem, vmem],
        scratch_shapes=[
            pltpu.VMEM((tok_rows, depth), bf16),
            parcels,
            parcels,
            parcels,
            parcels,
            pltpu.VMEM((depth, ff), bf16),
            pltpu.VMEM((depth, ff), bf16),
            pltpu.VMEM((ff, depth), bf16),
            pltpu.VMEM((GROUP * TILE, ff), bf16),
            pltpu.VMEM((GROUP * TILE, tail), bf16),
            pltpu.SemaphoreType.DMA((1,)),
            pltpu.SemaphoreType.DMA((3,)),
            pltpu.SemaphoreType.DMA((2,)),
            pltpu.SemaphoreType.DMA((n,)),
            pltpu.SemaphoreType.DMA((n,)),
            pltpu.SemaphoreType.DMA((n,)),
            pltpu.SemaphoreType.DMA((n,)),
        ],
        compiler_params=pltpu.CompilerParams(
            collective_id=0, has_side_effects=True, vmem_limit_bytes=56 * 1024 * 1024
        ),
        name="exchange_ffn",
    )(keys, keys.T, tokens, w_gate, w_up, w_down)
    return jnp.concatenate([head, ends], axis=1)


def plain(tokens, routed, slot, w_gate, w_up, w_down, experts, capacity):
    position = routed * capacity + slot
    outgoing = (
        jnp.zeros((experts * capacity, tokens.shape[1]), jnp.bfloat16).at[position].set(tokens)
    )
    parcel = lax.all_to_all(
        outgoing.reshape(experts, capacity, outgoing.shape[1]),
        ("pair", "ep"), split_axis=0, concat_axis=0, tiled=True,
    )
    flat_rows = parcel.reshape(experts * capacity, parcel.shape[2])
    gate_proj = dot(flat_rows, w_gate[0])
    up_proj = dot(flat_rows, w_up[0])
    hidden = (jax.nn.silu(gate_proj) * up_proj).astype(jnp.bfloat16)
    result = dot(hidden, w_down[0]).astype(jnp.bfloat16)
    returned = lax.all_to_all(
        result.reshape(experts, capacity, result.shape[1]),
        ("pair", "ep"), split_axis=0, concat_axis=0, tiled=True,
    )
    return jnp.take(returned.reshape(experts * capacity, -1), position, axis=0)


def shards(tokens, expert_of, w_gate, w_up, w_down):
    pairs = lax.axis_size("pair")
    eps = lax.axis_size("ep")
    experts = pairs * eps
    tok_rows, depth = tokens.shape
    cap = tok_rows // experts + tok_rows // (2 * experts)
    routed = expert_of[:, 0]
    onehot = (routed[:, None] == jnp.arange(experts, dtype=jnp.int32)[None, :]).astype(jnp.float32)
    order = jnp.arange(tok_rows)
    earlier = (order[:, None] > order[None, :]).astype(jnp.bfloat16)
    before = dot(earlier, onehot.astype(jnp.bfloat16))
    slot = jnp.sum(before * onehot, axis=1).astype(jnp.int32)
    spare = TILE - cap
    packs = 0 < spare <= cap and cap % spare == 0 and (depth * spare) % (TILE * 256) == 0
    if packs and experts % GROUP == 0 and w_gate.shape[2] % 256 == 0:
        return fused(tokens, routed, slot, w_gate, w_up, w_down, pairs, eps, cap)
    return plain(tokens, routed, slot, w_gate, w_up, w_down, experts, cap)


def solution(mesh):
    spec2 = P(("pair", "ep"), None)
    spec3 = P(("pair", "ep"), None, None)
    return jax.shard_map(
        shards,
        mesh=mesh,
        in_specs=(spec2, spec2, spec3, spec3, spec3),
        out_specs=spec2,
        check_vma=False,
    )
```
